32 devices in a mesh: row: 8 (over y, x, core), grp: 4 (over z).
Axes of the slice: x: 2, y: 2, z: 4, core: 2. Of those that a mesh axis runs over, the one named last changes fastest.
Arguments:
- positions: float32 [3, 1024], replicated, may hold values from -0.05 to 9.35, as said below
- detuning: float32 [1024], replicated, may hold values from -1 to 1
- populations: float32 [1024], P('row'), may hold values from 0 to 1
- base: float32 [2, 64, 1024], P(None, 'grp', 'row'), may hold values from -6 to 6
- section: float32 [2, 64, 1024], P(None, 'grp', 'row'), may hold values from -6 to 6
- accum: float32 [2, 64, 1024], P(None, 'grp', 'row'), may hold values from -3 to 3
Outputs:
- next_input: float32 [2, 64, 1024], P(None, 'grp', 'row')
- accum_out: float32 [2, 64, 1024], P(None, 'grp', 'row')
The draws below stay inside these ranges and needn't reach their ends.
Inputs may be any that keep to these rules, and one draw needn't show every extreme that they name: `positions`: emitter n sits near the lattice point 0.3 * (n % 32, (n // 32) % 32, n // 1024), displaced by at most 0.05 in each coordinate.
All inputs are finite; a program needn't handle non-finite values.
Results may differ from the reference program's by a relative error of at most 0.0003.
Values sent between devices are 32-bit elements; how exact they have to be, the bound alone decides.
A program may use at most 64 MiB of HBM per device.

```python
import math
import jax
import jax.numpy as jnp
from jax import lax

S = 64
N = 1024


def draw_positions(key, part):
    index = jnp.arange(N, dtype=jnp.int32)
    lattice = jnp.stack([index % 32, index // 32 % 32, index // 1024]).astype(jnp.float32) * 0.3
    jitter = jax.random.uniform(key, (3, N), jnp.float32, -0.05, 0.05)
    return lattice + jitter


def levels(own_key, extent, shards, low, high):
    def one(dim, shards_of):
        steps = jax.random.uniform(jax.random.fold_in(jax.random.fold_in(own_key, 6), dim), (shards_of,), jnp.float32, low / len(shards), high / len(shards))
        return jnp.repeat(jnp.exp(steps), extent[dim] // shards_of).reshape((-1,) + (1,) * (len(extent) - dim - 1))

    loudness = one(*shards[0])
    for cut in shards[1:]:
        loudness = loudness * one(*cut)
    return loudness


def centred(own_key, shape, spread, bound, cuts=(), held_as=jnp.bfloat16):
    array = jax.random.normal(own_key, shape, jnp.float32) * spread
    if len(cuts) > 0:
        array = levels(own_key, shape, cuts, -0.22, 0.18) * array
    return jnp.clip(array, min=-bound, max=bound).astype(held_as)


def setup_inputs(seed: int = 0) -> dict:
    seeds = jax.random.split(jax.random.key(seed), 7)
    positions = draw_positions(jax.random.fold_in(seeds[6], 71), 0)
    detuning = jnp.clip(jax.random.uniform(seeds[1], (N,), jnp.float32, -1.0, 1.0), -1.0, 1.0)
    populations = jnp.clip(1.0 * jax.random.uniform(seeds[2], (N,), jnp.float32) ** levels(seeds[2], (N,), ((0, 8),), -0.2, 0.2), 0.0, 1.0)
    base = centred(seeds[3], (2, S, N), 1.0, 6.0, ((1, 4), (2, 8)), jnp.float32)
    section = centred(seeds[4], (2, S, N), 1.0, 6.0, ((1, 4), (2, 8)), jnp.float32)
    accum = centred(seeds[5], (2, S, N), 0.5, 3.0, ((1, 4), (2, 8)), jnp.float32)
    return {"positions": positions, "detuning": detuning, "populations": populations, "base": base, "section": section, "accum": accum}


WAVE_NUMBER = 2.0 * math.pi
TIME_STEP = 0.2

def coupling(pos_rows, pos_cols, row_ids, col_ids):
    offsets = pos_rows[:, :, None] - pos_cols[:, None, :]
    dist_sq = lax.optimization_barrier(jnp.sum(offsets * offsets, axis=0))
    on_diag = row_ids[:, None] == col_ids[None, :]
    safe_sq = jnp.where(on_diag, 1.0, dist_sq)
    phase = WAVE_NUMBER * jnp.sqrt(safe_sq)
    inverse = 1.0 / phase
    inverse_sq = inverse * inverse
    aligned = offsets[2] * offsets[2] / safe_sq
    quad_real = 1.0 - inverse_sq - aligned * (1.0 - 3.0 * inverse_sq)
    quad_imag = inverse - 3.0 * aligned * inverse
    cosine = jnp.cos(phase)
    sine = jnp.sin(phase)
    h_real = -0.75 * inverse * (cosine * quad_real - sine * quad_imag)
    h_imag = -0.75 * inverse * (sine * quad_real + cosine * quad_imag)
    return (jnp.where(on_diag, 0.0, h_real), jnp.where(on_diag, 0.0, h_imag))

def cross_rows(slab_part, tile):
    return lax.dot_general(slab_part, tile, (((1,), (1,)), ((), ())), precision=lax.Precision.HIGHEST, preferred_element_type=jnp.float32)

def lead_rows(tile, slab_part):
    return lax.dot_general(tile, slab_part, (((0,), (0,)), ((), ())), precision=lax.Precision.HIGHEST, preferred_element_type=jnp.float32)

def slab_rate(z_real, z_imag, shift, local_slab, full_slab, local_det, slab_pos, slab_det, col_start, col_count):
    slab_ids = lax.iota(jnp.int32, slab_pos.shape[1])
    w_real, w_imag = coupling(slab_pos, slab_pos, slab_ids, slab_ids)
    eye_mask = slab_ids[:, None] == slab_ids[None, :]
    w_real = w_real + jnp.where(eye_mask, slab_det[:, None], 0.0)
    w_imag = w_imag + jnp.where(eye_mask, -0.5, 0.0)
    w_real = lax.dynamic_slice_in_dim(w_real, col_start, col_count, 1)
    w_imag = lax.dynamic_slice_in_dim(w_imag, col_start, col_count, 1)
    v_real = lead_rows(w_real, full_slab[0]) + lead_rows(w_imag, full_slab[1])
    v_imag = lead_rows(w_real, full_slab[1]) - lead_rows(w_imag, full_slab[0])
    y_real = local_slab[0]
    y_imag = local_slab[1]
    z_real = z_real + local_det * y_real + 0.5 * y_imag
    z_imag = z_imag + local_det * y_imag - 0.5 * y_real
    f_real = z_imag + shift * y_imag - v_imag
    f_imag = -z_real - shift * y_real + v_real
    return jnp.stack([f_real, f_imag])

def reference(positions, detuning, populations, base, section, accum):
    block_len = math.gcd(N, 512)
    block_total = N // block_len
    signed_pops = 2.0 * populations - 1.0
    all_ids = lax.iota(jnp.int32, N)

    def one_block(row_start):
        pos_rows = lax.dynamic_slice_in_dim(positions, row_start, block_len, 1)
        row_ids = row_start + lax.iota(jnp.int32, block_len)
        h_real, h_imag = coupling(pos_rows, positions, row_ids, all_ids)
        z_real = cross_rows(section[0], h_real) - cross_rows(section[1], h_imag)
        z_imag = cross_rows(section[0], h_imag) + cross_rows(section[1], h_real)
        shift = jnp.dot(h_real, signed_pops, precision=lax.Precision.HIGHEST)
        return (z_real, z_imag, shift)
    starts = (jnp.arange(block_total) * block_len).astype(jnp.int32)
    z_real, z_imag, shift = lax.map(one_block, starts)
    z_real = jnp.transpose(z_real, (1, 0, 2)).reshape(S, N)
    z_imag = jnp.transpose(z_imag, (1, 0, 2)).reshape(S, N)
    shift = shift.reshape(N)
    rate = slab_rate(z_real, z_imag, shift, section, section, detuning, positions[:, :S], detuning[:S], 0, S)
    return (base + 0.5 * TIME_STEP * rate, accum + TIME_STEP / 3.0 * rate)
```

```python
import functools
import math

import jax
import jax.numpy as jnp
from jax import lax
from jax.experimental import pallas as pl
from jax.experimental.pallas import tpu as pltpu
from jax.sharding import PartitionSpec as P

TIME_STEP = 0.2
CHUNK = 32
PAD = 16

SIN_COEFFS = (
    6.283185302511502,
    -41.3417004053172,
    81.60513138578366,
    -76.7030153536576,
    42.02592698454004,
    -14.89984666366821,
    3.2381375046186873,
)
COS_COEFFS = (
    0.9999999890590228,
    -19.739204499453827,
    64.9391174598908,
    -85.45013953079768,
    60.16763095026347,
    -25.967599245923736,
    6.52865815775625,
)


def horner(coeffs, t):
    total = coeffs[-1] * t + coeffs[-2]
    for value in coeffs[-3::-1]:
        total = total * t + value
    return total


def coupling(cols, rows, diag):
    dx = cols[0] - rows[0]
    dy = cols[1] - rows[1]
    dz = cols[2] - rows[2]
    dz_sq = dz * dz
    dist_sq = dx * dx + dy * dy + dz_sq
    if diag is not None:
        dist_sq = jnp.where(diag, 1.0, dist_sq)
    inv = lax.rsqrt(dist_sq)
    dist = dist_sq * inv
    frac = dist - jnp.round(dist)
    t = frac * frac
    sine = frac * horner(SIN_COEFFS, t)
    cosine = horner(COS_COEFFS, t)
    aligned = dz_sq * (inv * inv)
    mix = 1.0 - 3.0 * aligned
    u = inv * (0.5 / math.pi)
    quad_imag = u * mix
    quad_real = (1.0 - aligned) - u * quad_imag
    scale = -0.75 * u
    amp_real = scale * quad_real
    amp_imag = scale * quad_imag
    h_real = amp_real * cosine - amp_imag * sine
    h_imag = amp_real * sine + amp_imag * cosine
    if diag is not None:
        h_real = jnp.where(diag, 0.0, h_real)
        h_imag = jnp.where(diag, 0.0, h_imag)
    return h_real, h_imag


def split(x):
    hi = x.astype(jnp.bfloat16)
    return hi, (x - hi.astype(jnp.float32)).astype(jnp.bfloat16)


def bdot(a, b):
    return jnp.dot(a, b, preferred_element_type=jnp.float32)


def kernel(
    n_row,
    n_grp,
    early,
    pos_ref,
    det_ref,
    pop_ref,
    sec_ref,
    out_ref,
    pos_t,
    rhs_hi,
    rhs_lo,
    row_buf,
    pop_buf,
    grp_buf,
    sec_send,
    sec_recv,
    pop_send,
    pop_recv,
    grp_send,
    grp_recv,
):
    me = lax.axis_index("row")
    mine = lax.axis_index("grp")
    cols, width = sec_ref.shape[1], sec_ref.shape[2]
    slab = cols * n_grp

    def row_peer(s):
        return lax.rem(me + s, n_row)

    def grp_peer(s):
        return lax.rem(mine + s, n_grp)

    barrier = pltpu.get_barrier_semaphore()
    for s in range(1, n_row):
        pl.semaphore_signal(barrier, inc=1, device_id={"row": row_peer(s)}, device_id_type=pl.DeviceIdType.MESH)
    for s in range(1, n_grp):
        pl.semaphore_signal(barrier, inc=1, device_id={"grp": grp_peer(s)}, device_id_type=pl.DeviceIdType.MESH)

    for b in range(n_row):
        part = pos_ref[:, b * width : (b + 1) * width]
        tall = jnp.concatenate([part, jnp.zeros((5, width), jnp.float32)], axis=0)
        pos_t[b * width : (b + 1) * width, :] = jnp.transpose(tall)

    my_start = pl.multiple_of(me * width, width)
    rows = [pos_ref[d : d + 1, pl.ds(my_start, width)] for d in range(3)]
    chunks = width // CHUNK

    def fill(slot_row, pos_row, diag):
        block = pos_t[pl.ds(pos_row, CHUNK), :]
        h_real, h_imag = coupling([block[:, d : d + 1] for d in range(3)], rows, diag)
        for lane, h in ((0, h_real), (width, h_imag)):
            hi, lo = split(h)
            rhs_hi[pl.ds(slot_row, CHUNK), lane : lane + width] = hi
            rhs_lo[pl.ds(slot_row, CHUNK), lane : lane + width] = lo

    lane_ids = lax.broadcasted_iota(jnp.int32, (CHUNK, width), 1)
    sub_ids = lax.broadcasted_iota(jnp.int32, (CHUNK, width), 0)

    def own_chunk(j, carry):
        offset = pl.multiple_of(j * CHUNK, CHUNK)
        fill(offset, pl.multiple_of(my_start + offset, CHUNK), sub_ids + offset == lane_ids)
        return carry

    def other_chunk(j, carry):
        offset = pl.multiple_of(j * CHUNK, CHUNK)
        owner = lax.rem(me + n_row - j // chunks, n_row)
        start = owner * width + lax.rem(j, chunks) * CHUNK
        fill(offset, pl.multiple_of(start, CHUNK), None)
        return carry

    lax.fori_loop(0, chunks, own_chunk, 0)
    lax.fori_loop(chunks, early * chunks, other_chunk, 0)

    pl.semaphore_wait(barrier, n_row + n_grp - 2)

    row_copies = []
    for s in range(1, n_row):
        target = {"row": row_peer(s)}
        copy = pltpu.make_async_remote_copy(
            sec_ref, row_buf.at[s], sec_send.at[s], sec_recv.at[s], device_id=target, device_id_type=pl.DeviceIdType.MESH
        )
        copy.start()
        pop_copy = pltpu.make_async_remote_copy(
            pop_ref, pop_buf.at[s], pop_send.at[s], pop_recv.at[s], device_id=target, device_id_type=pl.DeviceIdType.MESH
        )
        pop_copy.start()
        row_copies.append((copy, pop_copy))
    grp_copies = []
    for s in range(1, n_grp):
        copy = pltpu.make_async_remote_copy(
            sec_ref,
            grp_buf.at[s],
            grp_send.at[s],
            grp_recv.at[s],
            device_id={"grp": grp_peer(s)},
            device_id_type=pl.DeviceIdType.MESH,
        )
        copy.start()
        grp_copies.append(copy)

    col_start = pl.multiple_of(mine * cols, cols)
    own_pos = pos_t[pl.ds(col_start, cols), :]
    own_cols = [own_pos[:, d : d + 1] for d in range(3)]
    slab_diag = lax.broadcasted_iota(jnp.int32, (cols, width), 0) + col_start == lax.broadcasted_iota(
        jnp.int32, (cols, width), 1
    )
    slab_rows = [pos_ref[d : d + 1, :width] for d in range(3)]
    w_real, w_imag = coupling(own_cols, slab_rows, slab_diag)
    w_real = w_real + jnp.where(slab_diag, det_ref[:, :width], 0.0)
    w_imag = w_imag + jnp.where(slab_diag, -0.5, 0.0)
    lead_all = jnp.concatenate([w_real, w_imag], axis=0)

    lax.fori_loop(early * chunks, n_row * chunks, other_chunk, 0)

    def left(sec, pop):
        signed = jnp.broadcast_to(2.0 * pop - 1.0, (PAD, width))
        return split(jnp.concatenate([sec[0], sec[1], signed], axis=0))

    y_local = sec_ref[...]
    main = jnp.zeros((4 * cols + 2 * PAD, 2 * width), jnp.float32)
    rest = jnp.zeros((2 * cols + PAD, 2 * width), jnp.float32)
    group = 2 if n_row % 2 == 0 else 1
    for first in range(0, n_row, group):
        his, los = [], []
        for s in range(first, first + group):
            if s == 0:
                hi, lo = left(y_local, pop_ref[...])
            else:
                row_copies[s - 1][0].wait_recv()
                row_copies[s - 1][1].wait_recv()
                hi, lo = left(row_buf[s], pop_buf[s])
            his.append(hi)
            los.append(lo)
        hi = jnp.concatenate(his, axis=1)
        lo = jnp.concatenate(los, axis=1)
        span = slice(first * width, (first + group) * width)
        main = main + bdot(jnp.concatenate([hi, lo], axis=0), rhs_hi[span, :])
        rest = rest + bdot(hi, rhs_lo[span, :])
    half = 2 * cols + PAD
    z = main[:half] + main[half:] + rest
    z_real = z[:cols, :width] - z[cols : 2 * cols, width:]
    z_imag = z[:cols, width:] + z[cols : 2 * cols, :width]
    shift = z[2 * cols : 2 * cols + 1, :width]

    for copy in grp_copies:
        copy.wait_recv()
    grp_buf[0] = y_local
    blocks = [grp_buf[lax.rem(mine + n_grp - g, n_grp)] for g in range(n_grp)]
    full = jnp.concatenate(
        [jnp.concatenate([block[0], block[1]], axis=1) for block in blocks], axis=0
    )
    f_hi, f_lo = split(full)
    l_hi, l_lo = split(lead_all[:, :slab])
    v = bdot(l_hi, f_hi) + bdot(l_lo, f_hi) + bdot(l_hi, f_lo)
    v_real = v[:cols, :width] + v[cols:, width:]
    v_imag = v[:cols, width:] - v[cols:, :width]

    y_real, y_imag = y_local[0], y_local[1]
    total_shift = shift + det_ref[:, pl.ds(my_start, width)]
    z_real = z_real + total_shift * y_real + 0.5 * y_imag
    z_imag = z_imag + total_shift * y_imag - 0.5 * y_real
    out_ref[0] = z_imag - v_imag
    out_ref[1] = v_real - z_real

    for copy, pop_copy in row_copies:
        copy.wait_send()
        pop_copy.wait_send()
    for copy in grp_copies:
        copy.wait_send()


def local(positions, detuning, populations, base, section, accum):
    n_row, n_grp = lax.axis_size("row"), lax.axis_size("grp")
    cols, width = section.shape[1], section.shape[2]
    total = positions.shape[1]
    block = section.shape
    rate = pl.pallas_call(
        functools.partial(kernel, n_row, n_grp, n_row // 2),
        out_shape=jax.ShapeDtypeStruct(block, jnp.float32),
        in_specs=[pl.BlockSpec(memory_space=pltpu.VMEM)] * 4,
        out_specs=pl.BlockSpec(memory_space=pltpu.VMEM),
        scratch_shapes=[
            pltpu.VMEM((total, 8), jnp.float32),
            pltpu.VMEM((total, 2 * width), jnp.bfloat16),
            pltpu.VMEM((total, 2 * width), jnp.bfloat16),
            pltpu.VMEM((n_row,) + block, jnp.float32),
            pltpu.VMEM((n_row, 1, width), jnp.float32),
            pltpu.VMEM((n_grp,) + block, jnp.float32),
            pltpu.SemaphoreType.DMA((n_row,)),
            pltpu.SemaphoreType.DMA((n_row,)),
            pltpu.SemaphoreType.DMA((n_row,)),
            pltpu.SemaphoreType.DMA((n_row,)),
            pltpu.SemaphoreType.DMA((n_grp,)),
            pltpu.SemaphoreType.DMA((n_grp,)),
        ],
        compiler_params=pltpu.CompilerParams(collective_id=0, has_side_effects=True),
    )(positions, detuning.reshape(1, total), populations.reshape(1, width), section)
    return (base + 0.5 * TIME_STEP * rate, accum + TIME_STEP / 3.0 * rate)


def solution(mesh):
    return jax.shard_map(
        local,
        mesh=mesh,
        in_specs=(
            P(),
            P(),
            P("row"),
            P(None, "grp", "row"),
            P(None, "grp", "row"),
            P(None, "grp", "row"),
        ),
        out_specs=(P(None, "grp", "row"), P(None, "grp", "row")),
        check_vma=False,
    )
```

```python
import functools
import math

import jax
import jax.numpy as jnp
from jax import lax
from jax.experimental import pallas as pl
from jax.experimental.pallas import tpu as pltpu
from jax.sharding import PartitionSpec as P

TIME_STEP = 0.2
CHUNK = 32
PAD = 16

SIN_COEFFS = (
    6.283185302511502,
    -41.3417004053172,
    81.60513138578366,
    -76.7030153536576,
    42.02592698454004,
    -14.89984666366821,
    3.2381375046186873,
)
COS_COEFFS = (
    0.9999999890590228,
    -19.739204499453827,
    64.9391174598908,
    -85.45013953079768,
    60.16763095026347,
    -25.967599245923736,
    6.52865815775625,
)


def horner(coeffs, t):
    total = coeffs[-1] * t + coeffs[-2]
    for value in coeffs[-3::-1]:
        total = total * t + value
    return total


def coupling(cols, rows, diag):
    dx = cols[0] - rows[0]
    dy = cols[1] - rows[1]
    dz = cols[2] - rows[2]
    dz_sq = dz * dz
    dist_sq = dx * dx + dy * dy + dz_sq
    if diag is not None:
        dist_sq = jnp.where(diag, 1.0, dist_sq)
    inv = lax.rsqrt(dist_sq)
    dist = dist_sq * inv
    frac = dist - jnp.round(dist)
    t = frac * frac
    sine = frac * horner(SIN_COEFFS, t)
    cosine = horner(COS_COEFFS, t)
    aligned = dz_sq * (inv * inv)
    mix = 1.0 - 3.0 * aligned
    u = inv * (0.5 / math.pi)
    quad_imag = u * mix
    quad_real = (1.0 - aligned) - u * quad_imag
    scale = -0.75 * u
    amp_real = scale * quad_real
    amp_imag = scale * quad_imag
    h_real = amp_real * cosine - amp_imag * sine
    h_imag = amp_real * sine + amp_imag * cosine
    if diag is not None:
        h_real = jnp.where(diag, 0.0, h_real)
        h_imag = jnp.where(diag, 0.0, h_imag)
    return h_real, h_imag


def split(x):
    hi = x.astype(jnp.bfloat16)
    return hi, (x - hi.astype(jnp.float32)).astype(jnp.bfloat16)


def bdot(a, b):
    return jnp.dot(a, b, preferred_element_type=jnp.float32)


def kernel(
    n_row,
    n_grp,
    pos_in,
    det_in,
    pop_in,
    sec_in,
    out_ref,
    pos_ref,
    det_ref,
    pop_ref,
    sec_ref,
    pos_t,
    rhs_hi,
    rhs_lo,
    row_buf,
    pop_buf,
    grp_buf,
    sec_send,
    sec_recv,
    pop_send,
    pop_recv,
    grp_send,
    grp_recv,
    load_sem,
):
    loads = []
    for i, (src, dst) in enumerate(((sec_in, sec_ref), (pop_in, pop_ref), (pos_in, pos_ref), (det_in, det_ref))):
        load = pltpu.make_async_copy(src, dst, load_sem.at[i])
        load.start()
        loads.append(load)
    me = lax.axis_index("row")
    mine = lax.axis_index("grp")
    cols, width = sec_ref.shape[1], sec_ref.shape[2]
    slab = cols * n_grp

    def row_peer(s):
        return lax.rem(me + s, n_row)

    def grp_peer(s):
        return lax.rem(mine + s, n_grp)

    barrier = pltpu.get_barrier_semaphore()
    for s in range(1, n_row):
        pl.semaphore_signal(barrier, inc=1, device_id={"row": row_peer(s)}, device_id_type=pl.DeviceIdType.MESH)
    for s in range(1, n_grp):
        pl.semaphore_signal(barrier, inc=1, device_id={"grp": grp_peer(s)}, device_id_type=pl.DeviceIdType.MESH)

    loads[0].wait()
    loads[1].wait()
    pl.semaphore_wait(barrier, n_row + n_grp - 2)

    row_copies = []
    for s in range(1, n_row):
        target = {"row": row_peer(s)}
        copy = pltpu.make_async_remote_copy(
            sec_ref, row_buf.at[s], sec_send.at[s], sec_recv.at[s], device_id=target, device_id_type=pl.DeviceIdType.MESH
        )
        copy.start()
        pop_copy = pltpu.make_async_remote_copy(
            pop_ref, pop_buf.at[s], pop_send.at[s], pop_recv.at[s], device_id=target, device_id_type=pl.DeviceIdType.MESH
        )
        pop_copy.start()
        row_copies.append((copy, pop_copy))
    grp_copies = []
    for s in range(1, n_grp):
        copy = pltpu.make_async_remote_copy(
            sec_ref,
            grp_buf.at[s],
            grp_send.at[s],
            grp_recv.at[s],
            device_id={"grp": grp_peer(s)},
            device_id_type=pl.DeviceIdType.MESH,
        )
        copy.start()
        grp_copies.append(copy)

    loads[2].wait()
    loads[3].wait()
    for b in range(n_row):
        part = pos_ref[:, b * width : (b + 1) * width]
        tall = jnp.concatenate([part, jnp.zeros((5, width), jnp.float32)], axis=0)
        pos_t[b * width : (b + 1) * width, :] = jnp.transpose(tall)

    my_start = pl.multiple_of(me * width, width)
    rows = [pos_ref[d : d + 1, pl.ds(my_start, width)] for d in range(3)]
    chunks = width // CHUNK

    def fill(slot_row, pos_row, diag):
        block = pos_t[pl.ds(pos_row, CHUNK), :]
        h_real, h_imag = coupling([block[:, d : d + 1] for d in range(3)], rows, diag)
        for lane, h in ((0, h_real), (width, h_imag)):
            hi, lo = split(h)
            rhs_hi[pl.ds(slot_row, CHUNK), lane : lane + width] = hi
            rhs_lo[pl.ds(slot_row, CHUNK), lane : lane + width] = lo

    lane_ids = lax.broadcasted_iota(jnp.int32, (CHUNK, width), 1)
    sub_ids = lax.broadcasted_iota(jnp.int32, (CHUNK, width), 0)

    def own_chunk(j, carry):
        offset = pl.multiple_of(j * CHUNK, CHUNK)
        fill(offset, pl.multiple_of(my_start + offset, CHUNK), sub_ids + offset == lane_ids)
        return carry

    def other_chunk(j, carry):
        offset = pl.multiple_of(j * CHUNK, CHUNK)
        owner = lax.rem(me + n_row - j // chunks, n_row)
        start = owner * width + lax.rem(j, chunks) * CHUNK
        fill(offset, pl.multiple_of(start, CHUNK), None)
        return carry

    lax.fori_loop(0, chunks, own_chunk, 0)

    col_start = pl.multiple_of(mine * cols, cols)
    own_pos = pos_t[pl.ds(col_start, cols), :]
    own_cols = [own_pos[:, d : d + 1] for d in range(3)]
    slab_diag = lax.broadcasted_iota(jnp.int32, (cols, width), 0) + col_start == lax.broadcasted_iota(
        jnp.int32, (cols, width), 1
    )
    slab_rows = [pos_ref[d : d + 1, :width] for d in range(3)]
    w_real, w_imag = coupling(own_cols, slab_rows, slab_diag)
    w_real = w_real + jnp.where(slab_diag, det_ref[:, :width], 0.0)
    w_imag = w_imag + jnp.where(slab_diag, -0.5, 0.0)
    lead_all = jnp.concatenate([w_real, w_imag], axis=0)

    lax.fori_loop(chunks, n_row * chunks, other_chunk, 0)

    def left(sec, pop):
        signed = jnp.broadcast_to(2.0 * pop - 1.0, (PAD, width))
        return split(jnp.concatenate([sec[0], sec[1], signed], axis=0))

    y_local = sec_ref[...]
    main = jnp.zeros((4 * cols + 2 * PAD, 2 * width), jnp.float32)
    rest = jnp.zeros((2 * cols + PAD, 2 * width), jnp.float32)
    group = 2 if n_row % 2 == 0 else 1
    for first in range(0, n_row, group):
        his, los = [], []
        for s in range(first, first + group):
            if s == 0:
                hi, lo = left(y_local, pop_ref[...])
            else:
                row_copies[s - 1][0].wait_recv()
                row_copies[s - 1][1].wait_recv()
                hi, lo = left(row_buf[s], pop_buf[s])
            his.append(hi)
            los.append(lo)
        hi = jnp.concatenate(his, axis=1)
        lo = jnp.concatenate(los, axis=1)
        span = slice(first * width, (first + group) * width)
        main = main + bdot(jnp.concatenate([hi, lo], axis=0), rhs_hi[span, :])
        rest = rest + bdot(hi, rhs_lo[span, :])
    half = 2 * cols + PAD
    z = main[:half] + main[half:] + rest
    z_real = z[:cols, :width] - z[cols : 2 * cols, width:]
    z_imag = z[:cols, width:] + z[cols : 2 * cols, :width]
    shift = z[2 * cols : 2 * cols + 1, :width]

    for copy in grp_copies:
        copy.wait_recv()
    grp_buf[0] = y_local
    blocks = [grp_buf[lax.rem(mine + n_grp - g, n_grp)] for g in range(n_grp)]
    full = jnp.concatenate(
        [jnp.concatenate([block[0], block[1]], axis=1) for block in blocks], axis=0
    )
    f_hi, f_lo = split(full)
    l_hi, l_lo = split(lead_all[:, :slab])
    v = bdot(l_hi, f_hi) + bdot(l_lo, f_hi) + bdot(l_hi, f_lo)
    v_real = v[:cols, :width] + v[cols:, width:]
    v_imag = v[:cols, width:] - v[cols:, :width]

    y_real, y_imag = y_local[0], y_local[1]
    total_shift = shift + det_ref[:, pl.ds(my_start, width)]
    z_real = z_real + total_shift * y_real + 0.5 * y_imag
    z_imag = z_imag + total_shift * y_imag - 0.5 * y_real
    out_ref[0] = z_imag - v_imag
    out_ref[1] = v_real - z_real

    for copy, pop_copy in row_copies:
        copy.wait_send()
        pop_copy.wait_send()
    for copy in grp_copies:
        copy.wait_send()


def local(positions, detuning, populations, base, section, accum):
    n_row, n_grp = lax.axis_size("row"), lax.axis_size("grp")
    cols, width = section.shape[1], section.shape[2]
    total = positions.shape[1]
    block = section.shape
    rate = pl.pallas_call(
        functools.partial(kernel, n_row, n_grp),
        out_shape=pltpu.VMEM(block, jnp.float32),
        in_specs=[pl.BlockSpec(memory_space=pl.ANY)] * 4,
        out_specs=pl.BlockSpec(memory_space=pltpu.VMEM),
        scratch_shapes=[
            pltpu.VMEM((3, total), jnp.float32),
            pltpu.VMEM((1, total), jnp.float32),
            pltpu.VMEM((1, width), jnp.float32),
            pltpu.VMEM(block, jnp.float32),
            pltpu.VMEM((total, 8), jnp.float32),
            pltpu.VMEM((total, 2 * width), jnp.bfloat16),
            pltpu.VMEM((total, 2 * width), jnp.bfloat16),
            pltpu.VMEM((n_row,) + block, jnp.float32),
            pltpu.VMEM((n_row, 1, width), jnp.float32),
            pltpu.VMEM((n_grp,) + block, jnp.float32),
            pltpu.SemaphoreType.DMA((n_row,)),
            pltpu.SemaphoreType.DMA((n_row,)),
            pltpu.SemaphoreType.DMA((n_row,)),
            pltpu.SemaphoreType.DMA((n_row,)),
            pltpu.SemaphoreType.DMA((n_grp,)),
            pltpu.SemaphoreType.DMA((n_grp,)),
            pltpu.SemaphoreType.DMA((4,)),
        ],
        compiler_params=pltpu.CompilerParams(collective_id=0, has_side_effects=True),
    )(positions, detuning.reshape(1, total), populations.reshape(1, width), section)
    return (base + 0.5 * TIME_STEP * rate, accum + TIME_STEP / 3.0 * rate)


def solution(mesh):
    return jax.shard_map(
        local,
        mesh=mesh,
        in_specs=(
            P(),
            P(),
            P("row"),
            P(None, "grp", "row"),
            P(None, "grp", "row"),
            P(None, "grp", "row"),
        ),
        out_specs=(P(None, "grp", "row"), P(None, "grp", "row")),
        check_vma=False,
    )
```

```python
import functools
import math

import jax
import jax.numpy as jnp
from jax import lax
from jax.experimental import pallas as pl
from jax.experimental.pallas import tpu as pltpu
from jax.sharding import PartitionSpec as P

TIME_STEP = 0.2
CHUNK = 32
PAD = 16

SIN_COEFFS = (
    6.283185302511502,
    -41.3417004053172,
    81.60513138578366,
    -76.7030153536576,
    42.02592698454004,
    -14.89984666366821,
    3.2381375046186873,
)
COS_COEFFS = (
    0.9999999890590228,
    -19.739204499453827,
    64.9391174598908,
    -85.45013953079768,
    60.16763095026347,
    -25.967599245923736,
    6.52865815775625,
)


def horner(coeffs, t):
    total = coeffs[-1] * t + coeffs[-2]
    for value in coeffs[-3::-1]:
        total = total * t + value
    return total


def coupling(cols, rows, diag):
    dx = cols[0] - rows[0]
    dy = cols[1] - rows[1]
    dz = cols[2] - rows[2]
    dz_sq = dz * dz
    dist_sq = dx * dx + dy * dy + dz_sq
    if diag is not None:
        dist_sq = jnp.where(diag, 1.0, dist_sq)
    inv = lax.rsqrt(dist_sq)
    dist = dist_sq * inv
    frac = dist - jnp.round(dist)
    t = frac * frac
    sine = frac * horner(SIN_COEFFS, t)
    cosine = horner(COS_COEFFS, t)
    aligned = dz_sq * (inv * inv)
    mix = 1.0 - 3.0 * aligned
    u = inv * (0.5 / math.pi)
    quad_imag = u * mix
    quad_real = (1.0 - aligned) - u * quad_imag
    scale = -0.75 * u
    amp_real = scale * quad_real
    amp_imag = scale * quad_imag
    h_real = amp_real * cosine - amp_imag * sine
    h_imag = amp_real * sine + amp_imag * cosine
    if diag is not None:
        h_real = jnp.where(diag, 0.0, h_real)
        h_imag = jnp.where(diag, 0.0, h_imag)
    return h_real, h_imag


def split(x):
    hi = x.astype(jnp.bfloat16)
    return hi, (x - hi.astype(jnp.float32)).astype(jnp.bfloat16)


def bdot(a, b):
    return jnp.dot(a, b, preferred_element_type=jnp.float32)


def kernel(
    n_row,
    n_grp,
    pos_in,
    det_in,
    pop_in,
    sec_in,
    out_ref,
    pos_ref,
    det_ref,
    stage,
    pos_t,
    rhs_hi,
    rhs_lo,
    row_buf,
    grp_buf,
    sec_send,
    sec_recv,
    grp_send,
    grp_recv,
    load_sem,
):
    cols, width = sec_in.shape[1], sec_in.shape[2]
    loads = []
    for i, (src, dst) in enumerate(
        (
            (sec_in.at[0], stage.at[0:cols]),
            (sec_in.at[1], stage.at[cols : 2 * cols]),
            (pop_in, stage.at[2 * cols : 2 * cols + 1]),
            (pos_in, pos_ref),
            (det_in, det_ref),
        )
    ):
        load = pltpu.make_async_copy(src, dst, load_sem.at[i])
        load.start()
        loads.append(load)
    me = lax.axis_index("row")
    mine = lax.axis_index("grp")
    slab = cols * n_grp

    def row_peer(s):
        return lax.rem(me + s, n_row)

    def grp_peer(s):
        return lax.rem(mine + s, n_grp)

    barrier = pltpu.get_barrier_semaphore()
    for s in range(1, n_grp):
        pl.semaphore_signal(barrier, inc=1, device_id={"grp": grp_peer(s)}, device_id_type=pl.DeviceIdType.MESH)
    for s in range(1, n_row):
        pl.semaphore_signal(barrier, inc=1, device_id={"row": row_peer(s)}, device_id_type=pl.DeviceIdType.MESH)

    loads[0].wait()
    loads[1].wait()
    pl.semaphore_wait(barrier, n_row + n_grp - 2)

    slab_part = stage.at[0 : 2 * cols]
    grp_copies = []
    for s in range(1, n_grp):
        copy = pltpu.make_async_remote_copy(
            slab_part,
            grp_buf.at[s],
            grp_send.at[s],
            grp_recv.at[s],
            device_id={"grp": grp_peer(s)},
            device_id_type=pl.DeviceIdType.MESH,
        )
        copy.start()
        grp_copies.append(copy)
    loads[2].wait()
    row_copies = []
    for s in range(n_row - 1, 0, -1):
        copy = pltpu.make_async_remote_copy(
            stage,
            row_buf.at[s],
            sec_send.at[s],
            sec_recv.at[s],
            device_id={"row": row_peer(s)},
            device_id_type=pl.DeviceIdType.MESH,
        )
        copy.start()
        row_copies.insert(0, copy)

    loads[3].wait()
    loads[4].wait()
    for b in range(n_row):
        part = pos_ref[:, b * width : (b + 1) * width]
        tall = jnp.concatenate([part, jnp.zeros((5, width), jnp.float32)], axis=0)
        pos_t[b * width : (b + 1) * width, :] = jnp.transpose(tall)

    my_start = pl.multiple_of(me * width, width)
    rows = [pos_ref[d : d + 1, pl.ds(my_start, width)] for d in range(3)]
    chunks = width // CHUNK

    def fill(slot_row, pos_row, diag):
        block = pos_t[pl.ds(pos_row, CHUNK), :]
        h_real, h_imag = coupling([block[:, d : d + 1] for d in range(3)], rows, diag)
        for lane, h in ((0, h_real), (width, h_imag)):
            hi, lo = split(h)
            rhs_hi[pl.ds(slot_row, CHUNK), lane : lane + width] = hi
            rhs_lo[pl.ds(slot_row, CHUNK), lane : lane + width] = lo

    lane_ids = lax.broadcasted_iota(jnp.int32, (CHUNK, width), 1)
    sub_ids = lax.broadcasted_iota(jnp.int32, (CHUNK, width), 0)

    def own_chunk(j, carry):
        offset = pl.multiple_of(j * CHUNK, CHUNK)
        fill(offset, pl.multiple_of(my_start + offset, CHUNK), sub_ids + offset == lane_ids)
        return carry

    def other_chunk(j, carry):
        offset = pl.multiple_of(j * CHUNK, CHUNK)
        owner = lax.rem(me + n_row - j // chunks, n_row)
        start = owner * width + lax.rem(j, chunks) * CHUNK
        fill(offset, pl.multiple_of(start, CHUNK), None)
        return carry

    lax.fori_loop(0, chunks, own_chunk, 0)

    col_start = pl.multiple_of(mine * cols, cols)
    own_pos = pos_t[pl.ds(col_start, cols), :]
    own_cols = [own_pos[:, d : d + 1] for d in range(3)]
    slab_diag = lax.broadcasted_iota(jnp.int32, (cols, width), 0) + col_start == lax.broadcasted_iota(
        jnp.int32, (cols, width), 1
    )
    slab_rows = [pos_ref[d : d + 1, :width] for d in range(3)]
    w_real, w_imag = coupling(own_cols, slab_rows, slab_diag)
    w_real = w_real + jnp.where(slab_diag, det_ref[:, :width], 0.0)
    w_imag = w_imag + jnp.where(slab_diag, -0.5, 0.0)
    lead_all = jnp.concatenate([w_real, w_imag], axis=0)

    lax.fori_loop(chunks, n_row * chunks, other_chunk, 0, unroll=2)

    def left(slab_and_pop):
        signed = jnp.broadcast_to(2.0 * slab_and_pop[2 * cols :] - 1.0, (PAD, width))
        return split(jnp.concatenate([slab_and_pop[: 2 * cols], signed], axis=0))

    y_local = stage[0 : 2 * cols]
    main = jnp.zeros((4 * cols + 2 * PAD, 2 * width), jnp.float32)
    rest = jnp.zeros((2 * cols + PAD, 2 * width), jnp.float32)
    group = 2 if n_row % 2 == 0 else 1
    for first in range(0, n_row, group):
        his, los = [], []
        for s in range(first, first + group):
            if s == 0:
                hi, lo = left(stage[...])
            else:
                row_copies[s - 1].wait_recv()
                hi, lo = left(row_buf[s])
            his.append(hi)
            los.append(lo)
        hi = jnp.concatenate(his, axis=1)
        lo = jnp.concatenate(los, axis=1)
        span = slice(first * width, (first + group) * width)
        main = main + bdot(jnp.concatenate([hi, lo], axis=0), rhs_hi[span, :])
        rest = rest + bdot(hi, rhs_lo[span, :])
    half = 2 * cols + PAD
    z = main[:half] + main[half:] + rest
    z_real = z[:cols, :width] - z[cols : 2 * cols, width:]
    z_imag = z[:cols, width:] + z[cols : 2 * cols, :width]
    shift = z[2 * cols : 2 * cols + 1, :width]

    for copy in grp_copies:
        copy.wait_recv()
    grp_buf[0] = y_local
    blocks = [grp_buf[lax.rem(mine + n_grp - g, n_grp)] for g in range(n_grp)]
    full = jnp.concatenate(
        [jnp.concatenate([block[:cols], block[cols:]], axis=1) for block in blocks], axis=0
    )
    f_hi, f_lo = split(full)
    l_hi, l_lo = split(lead_all[:, :slab])
    v = bdot(l_hi, f_hi) + bdot(l_lo, f_hi) + bdot(l_hi, f_lo)
    v_real = v[:cols, :width] + v[cols:, width:]
    v_imag = v[:cols, width:] - v[cols:, :width]

    y_real, y_imag = y_local[:cols], y_local[cols:]
    total_shift = shift + det_ref[:, pl.ds(my_start, width)]
    z_real = z_real + total_shift * y_real + 0.5 * y_imag
    z_imag = z_imag + total_shift * y_imag - 0.5 * y_real
    out_ref[0] = z_imag - v_imag
    out_ref[1] = v_real - z_real

    for copy in row_copies + grp_copies:
        copy.wait_send()


def local(positions, detuning, populations, base, section, accum):
    n_row, n_grp = lax.axis_size("row"), lax.axis_size("grp")
    cols, width = section.shape[1], section.shape[2]
    total = positions.shape[1]
    block = section.shape
    rate = pl.pallas_call(
        functools.partial(kernel, n_row, n_grp),
        out_shape=pltpu.VMEM(block, jnp.float32),
        in_specs=[pl.BlockSpec(memory_space=pl.ANY)] * 4,
        out_specs=pl.BlockSpec(memory_space=pltpu.VMEM),
        scratch_shapes=[
            pltpu.VMEM((3, total), jnp.float32),
            pltpu.VMEM((1, total), jnp.float32),
            pltpu.VMEM((2 * cols + 1, width), jnp.float32),
            pltpu.VMEM((total, 8), jnp.float32),
            pltpu.VMEM((total, 2 * width), jnp.bfloat16),
            pltpu.VMEM((total, 2 * width), jnp.bfloat16),
            pltpu.VMEM((n_row, 2 * cols + 1, width), jnp.float32),
            pltpu.VMEM((n_grp, 2 * cols, width), jnp.float32),
            pltpu.SemaphoreType.DMA((n_row,)),
            pltpu.SemaphoreType.DMA((n_row,)),
            pltpu.SemaphoreType.DMA((n_grp,)),
            pltpu.SemaphoreType.DMA((n_grp,)),
            pltpu.SemaphoreType.DMA((5,)),
        ],
        compiler_params=pltpu.CompilerParams(collective_id=0, has_side_effects=True),
    )(positions, detuning.reshape(1, total), populations.reshape(1, width), section)
    return (base + 0.5 * TIME_STEP * rate, accum + TIME_STEP / 3.0 * rate)


def solution(mesh):
    return jax.shard_map(
        local,
        mesh=mesh,
        in_specs=(
            P(),
            P(),
            P("row"),
            P(None, "grp", "row"),
            P(None, "grp", "row"),
            P(None, "grp", "row"),
        ),
        out_specs=(P(None, "grp", "row"), P(None, "grp", "row")),
        check_vma=False,
    )
```

```python
import functools
import math

import jax
import jax.numpy as jnp
from jax import lax
from jax.experimental import pallas as pl
from jax.experimental.pallas import tpu as pltpu
from jax.sharding import PartitionSpec as P

TIME_STEP = 0.2
CHUNK = 32
PAD = 16

SIN_COEFFS = (
    6.283185302511502,
    -41.3417004053172,
    81.60513138578366,
    -76.7030153536576,
    42.02592698454004,
    -14.89984666366821,
    3.2381375046186873,
)
COS_COEFFS = (
    0.9999999890590228,
    -19.739204499453827,
    64.9391174598908,
    -85.45013953079768,
    60.16763095026347,
    -25.967599245923736,
    6.52865815775625,
)


def horner(coeffs, t):
    total = coeffs[-1] * t + coeffs[-2]
    for value in coeffs[-3::-1]:
        total = total * t + value
    return total


def coupling(cols, rows, diag):
    dx = cols[0] - rows[0]
    dy = cols[1] - rows[1]
    dz = cols[2] - rows[2]
    dz_sq = dz * dz
    dist_sq = dx * dx + dy * dy + dz_sq
    if diag is not None:
        dist_sq = jnp.where(diag, 1.0, dist_sq)
    inv = lax.rsqrt(dist_sq)
    dist = dist_sq * inv
    frac = dist - jnp.round(dist)
    t = frac * frac
    sine = frac * horner(SIN_COEFFS, t)
    cosine = horner(COS_COEFFS, t)
    aligned = dz_sq * (inv * inv)
    mix = 1.0 - 3.0 * aligned
    u = inv * (0.5 / math.pi)
    quad_imag = u * mix
    quad_real = (1.0 - aligned) - u * quad_imag
    scale = -0.75 * u
    amp_real = scale * quad_real
    amp_imag = scale * quad_imag
    h_real = amp_real * cosine - amp_imag * sine
    h_imag = amp_real * sine + amp_imag * cosine
    if diag is not None:
        h_real = jnp.where(diag, 0.0, h_real)
        h_imag = jnp.where(diag, 0.0, h_imag)
    return h_real, h_imag


def split(x):
    hi = x.astype(jnp.bfloat16)
    return hi, (x - hi.astype(jnp.float32)).astype(jnp.bfloat16)


def bdot(a, b):
    return jnp.dot(a, b, preferred_element_type=jnp.float32)


def kernel(
    n_row,
    n_grp,
    pos_in,
    det_in,
    pop_in,
    sec_in,
    out_ref,
    pos_ref,
    det_ref,
    stage,
    pos_t,
    rhs_hi,
    rhs_lo,
    row_buf,
    grp_buf,
    sec_send,
    sec_recv,
    grp_send,
    grp_recv,
    load_sem,
):
    cols, width = sec_in.shape[1], sec_in.shape[2]
    loads = []
    for i, (src, dst) in enumerate(
        (
            (sec_in.at[0], stage.at[0:cols]),
            (sec_in.at[1], stage.at[cols : 2 * cols]),
            (pop_in, stage.at[2 * cols : 2 * cols + 1]),
            (pos_in, pos_ref),
            (det_in, det_ref),
        )
    ):
        load = pltpu.make_async_copy(src, dst, load_sem.at[i])
        load.start()
        loads.append(load)
    me = lax.axis_index("row")
    mine = lax.axis_index("grp")
    slab = cols * n_grp

    def row_peer(s):
        return lax.rem(me + s, n_row)

    def grp_peer(s):
        return lax.rem(mine + s, n_grp)

    barrier = pltpu.get_barrier_semaphore()
    for s in range(1, n_row):
        pl.semaphore_signal(barrier, inc=1, device_id={"row": row_peer(s)}, device_id_type=pl.DeviceIdType.MESH)
    for s in range(1, n_grp):
        pl.semaphore_signal(barrier, inc=1, device_id={"grp": grp_peer(s)}, device_id_type=pl.DeviceIdType.MESH)

    loads[0].wait()
    loads[1].wait()
    pl.semaphore_wait(barrier, n_row + n_grp - 2)

    loads[2].wait()
    row_copies = {}
    for s in range(1, n_row):
        copy = pltpu.make_async_remote_copy(
            stage,
            row_buf.at[s],
            sec_send.at[s],
            sec_recv.at[s],
            device_id={"row": row_peer(s)},
            device_id_type=pl.DeviceIdType.MESH,
        )
        copy.start()
        row_copies[s] = copy
    slab_part = stage.at[0 : 2 * cols]
    grp_copies = []
    for s in range(1, n_grp):
        copy = pltpu.make_async_remote_copy(
            slab_part,
            grp_buf.at[s],
            grp_send.at[s],
            grp_recv.at[s],
            device_id={"grp": grp_peer(s)},
            device_id_type=pl.DeviceIdType.MESH,
        )
        copy.start()
        grp_copies.append(copy)

    loads[3].wait()
    loads[4].wait()
    for b in range(n_row):
        part = pos_ref[:, b * width : (b + 1) * width]
        tall = jnp.concatenate([part, jnp.zeros((5, width), jnp.float32)], axis=0)
        pos_t[b * width : (b + 1) * width, :] = jnp.transpose(tall)

    my_start = pl.multiple_of(me * width, width)
    rows = [pos_ref[d : d + 1, pl.ds(my_start, width)] for d in range(3)]
    chunks = width // CHUNK

    def fill(slot_row, pos_row, diag):
        block = pos_t[pl.ds(pos_row, CHUNK), :]
        h_real, h_imag = coupling([block[:, d : d + 1] for d in range(3)], rows, diag)
        for lane, h in ((0, h_real), (width, h_imag)):
            hi, lo = split(h)
            rhs_hi[pl.ds(slot_row, CHUNK), lane : lane + width] = hi
            rhs_lo[pl.ds(slot_row, CHUNK), lane : lane + width] = lo

    lane_ids = lax.broadcasted_iota(jnp.int32, (CHUNK, width), 1)
    sub_ids = lax.broadcasted_iota(jnp.int32, (CHUNK, width), 0)

    def own_chunk(j, carry):
        offset = pl.multiple_of(j * CHUNK, CHUNK)
        fill(offset, pl.multiple_of(my_start + offset, CHUNK), sub_ids + offset == lane_ids)
        return carry

    def other_chunk(j, carry):
        offset = pl.multiple_of(j * CHUNK, CHUNK)
        owner = lax.rem(me + n_row - j // chunks, n_row)
        start = owner * width + lax.rem(j, chunks) * CHUNK
        fill(offset, pl.multiple_of(start, CHUNK), None)
        return carry

    lax.fori_loop(0, chunks, own_chunk, 0)

    col_start = pl.multiple_of(mine * cols, cols)
    own_pos = pos_t[pl.ds(col_start, cols), :]
    own_cols = [own_pos[:, d : d + 1] for d in range(3)]
    slab_diag = lax.broadcasted_iota(jnp.int32, (cols, width), 0) + col_start == lax.broadcasted_iota(
        jnp.int32, (cols, width), 1
    )
    slab_rows = [pos_ref[d : d + 1, :width] for d in range(3)]
    w_real, w_imag = coupling(own_cols, slab_rows, slab_diag)
    w_real = w_real + jnp.where(slab_diag, det_ref[:, :width], 0.0)
    w_imag = w_imag + jnp.where(slab_diag, -0.5, 0.0)
    lead_all = jnp.concatenate([w_real, w_imag], axis=0)

    lax.fori_loop(chunks, n_row * chunks, other_chunk, 0, unroll=2)

    def left(slab_and_pop):
        signed = jnp.broadcast_to(2.0 * slab_and_pop[2 * cols :] - 1.0, (PAD, width))
        return split(jnp.concatenate([slab_and_pop[: 2 * cols], signed], axis=0))

    y_local = stage[0 : 2 * cols]
    main = jnp.zeros((4 * cols + 2 * PAD, 2 * width), jnp.float32)
    rest = jnp.zeros((2 * cols + PAD, 2 * width), jnp.float32)
    group = 2 if n_row % 2 == 0 else 1
    for first in range(0, n_row, group):
        his, los = [], []
        for s in range(first, first + group):
            if s == 0:
                hi, lo = left(stage[...])
            else:
                row_copies[s].wait_recv()
                hi, lo = left(row_buf[s])
            his.append(hi)
            los.append(lo)
        hi = jnp.concatenate(his, axis=1)
        lo = jnp.concatenate(los, axis=1)
        span = slice(first * width, (first + group) * width)
        main = main + bdot(jnp.concatenate([hi, lo], axis=0), rhs_hi[span, :])
        rest = rest + bdot(hi, rhs_lo[span, :])
    half = 2 * cols + PAD
    z = main[:half] + main[half:] + rest
    z_real = z[:cols, :width] - z[cols : 2 * cols, width:]
    z_imag = z[:cols, width:] + z[cols : 2 * cols, :width]
    shift = z[2 * cols : 2 * cols + 1, :width]

    for copy in grp_copies:
        copy.wait_recv()
    grp_buf[0] = y_local
    blocks = [grp_buf[lax.rem(mine + n_grp - g, n_grp)] for g in range(n_grp)]
    full = jnp.concatenate(
        [jnp.concatenate([block[:cols], block[cols:]], axis=1) for block in blocks], axis=0
    )
    f_hi, f_lo = split(full)
    l_hi, l_lo = split(lead_all[:, :slab])
    v = bdot(l_hi, f_hi) + bdot(l_lo, f_hi) + bdot(l_hi, f_lo)
    v_real = v[:cols, :width] + v[cols:, width:]
    v_imag = v[:cols, width:] - v[cols:, :width]

    y_real, y_imag = y_local[:cols], y_local[cols:]
    total_shift = shift + det_ref[:, pl.ds(my_start, width)]
    z_real = z_real + total_shift * y_real + 0.5 * y_imag
    z_imag = z_imag + total_shift * y_imag - 0.5 * y_real
    out_ref[0] = z_imag - v_imag
    out_ref[1] = v_real - z_real

    for copy in list(row_copies.values()) + grp_copies:
        copy.wait_send()


def local(positions, detuning, populations, base, section, accum):
    n_row, n_grp = lax.axis_size("row"), lax.axis_size("grp")
    cols, width = section.shape[1], section.shape[2]
    total = positions.shape[1]
    block = section.shape
    rate = pl.pallas_call(
        functools.partial(kernel, n_row, n_grp),
        out_shape=pltpu.VMEM(block, jnp.float32),
        in_specs=[pl.BlockSpec(memory_space=pl.ANY)] * 4,
        out_specs=pl.BlockSpec(memory_space=pltpu.VMEM),
        scratch_shapes=[
            pltpu.VMEM((3, total), jnp.float32),
            pltpu.VMEM((1, total), jnp.float32),
            pltpu.VMEM((2 * cols + 1, width), jnp.float32),
            pltpu.VMEM((total, 8), jnp.float32),
            pltpu.VMEM((total, 2 * width), jnp.bfloat16),
            pltpu.VMEM((total, 2 * width), jnp.bfloat16),
            pltpu.VMEM((n_row, 2 * cols + 1, width), jnp.float32),
            pltpu.VMEM((n_grp, 2 * cols, width), jnp.float32),
            pltpu.SemaphoreType.DMA((n_row,)),
            pltpu.SemaphoreType.DMA((n_row,)),
            pltpu.SemaphoreType.DMA((n_grp,)),
            pltpu.SemaphoreType.DMA((n_grp,)),
            pltpu.SemaphoreType.DMA((5,)),
        ],
        compiler_params=pltpu.CompilerParams(collective_id=0, has_side_effects=True),
    )(positions, detuning.reshape(1, total), populations.reshape(1, width), section)
    return (base + 0.5 * TIME_STEP * rate, accum + TIME_STEP / 3.0 * rate)


def solution(mesh):
    return jax.shard_map(
        local,
        mesh=mesh,
        in_specs=(
            P(),
            P(),
            P("row"),
            P(None, "grp", "row"),
            P(None, "grp", "row"),
            P(None, "grp", "row"),
        ),
        out_specs=(P(None, "grp", "row"), P(None, "grp", "row")),
        check_vma=False,
    )
```
